32 devices in a mesh: replica: 2 (over x), tp: 8 (over z, y), sub: 2 (over core).
Axes of the slice: x: 2, y: 2, z: 4, core: 2. Of those that a mesh axis runs over, the one named last changes fastest.
Arguments:
- hidden_in: bfloat16 [8, 8192], P('replica'), parts along dimension 0, may hold values from -6 to 6
- norm_gain: float32 [16384], P('replica'), parts along dimension 0, may hold values from 0.1 to 1.9
- wqkv_old: bfloat16 [16, 2, 1280, 4096], P(('replica', 'tp'), 'sub'), parts along dimension 0, may hold values from -0.1875 to 0.1875
- wo: bfloat16 [16384, 8192], P(('replica', 'tp', 'sub')), parts along dimension 0, may hold values from -0.0625 to 0.0625
- key_cache: bfloat16 [8, 4096, 1024], P('replica', ('tp', 'sub')), parts along dimension 0, may hold values from -240 to 240
- value_cache: bfloat16 [8, 4096, 1024], P('replica', ('tp', 'sub')), parts along dimension 0, may hold values from -6 to 6
- lengths: int32 [8], P('replica'), parts along dimension 0, may hold values from 1 to 4096
- section_order: int32 [32], P('replica'), parts along dimension 0, may hold values from 0 to 15, each once
Outputs:
- mixed_out: bfloat16 [8, 8192], P('replica'), parts along dimension 0
- wqkv_new: bfloat16 [16, 2, 640, 8192], P(('replica', 'tp'), 'sub'), parts along dimension 0
The draws below stay inside these ranges and needn't reach their ends.
There are 2 independent parts, one for each index of `replica`. The reference program is written for one: setup_inputs(seed, part) draws one part's arguments, and reference() takes and returns one part's arrays. A program takes and returns all parts, laid end to end along the dimension named above; each array names one. Nothing has to cross between parts.
Inputs may be any that keep to these rules, and one draw needn't show every extreme that they name: `section_order`: each input row block appears once. The new token's position is lengths[b].
All inputs are finite; a program needn't handle non-finite values.
Results may differ from the reference program's by a relative error of at most 0.0085.
The reference program's roundings to bfloat16 on the way (of `full_t`, `normed`, `projected` and `attended`) count: a program that leaves them out, or rounds other values in their place, can miss the bound.
Values may be sent and summed in bfloat16 or wider, within the bound.
A program may use at most 128 MiB of HBM per device.

```python
import math
import jax
import jax.numpy as jnp
from jax import lax

D = 8192
HEADS = 64
KV_HEADS = 8
HEAD_DIM = 128
RANKS = 8
ROW_BLOCKS = 16
SEQS = 4
CACHE_LEN = 4096
QKV = 10240
RANK_COLS = 1280
COLS_DEV = 640
ROWS_OLD = 4096
BLOCK_ROWS = 512
N_TP = 8


def draw_key_cache(key, part):
    base = jax.random.normal(jax.random.fold_in(key, 11), (SEQS, CACHE_LEN, KV_HEADS * HEAD_DIM), jnp.float32)
    return jnp.clip(base, -6.0, 6.0).astype(jnp.bfloat16)


def place_ends(entries, key, smallest, top_value):
    spot = [jax.random.randint(jax.random.fold_in(key, axis), (), 0, length) for axis, length in enumerate(entries.shape)]
    widest = entries.shape.index(max(entries.shape))
    neighbour = spot[:widest] + [(spot[widest] + 1) % entries.shape[widest]] + spot[widest + 1:]
    return entries.at[tuple(spot)].set(smallest).at[tuple(neighbour)].set(top_value)


def level_of(key, extent, split, smallest, high):
    gain = 1.0
    for dim, shards_of in split:
        steps = jax.random.uniform(jax.random.fold_in(jax.random.fold_in(key, 6), dim), (shards_of,), jnp.float32, smallest / len(split), high / len(split))
        gain = gain * jnp.repeat(jnp.exp(steps), extent[dim] // shards_of).reshape((-1,) + (1,) * (len(extent) - 1 - dim))
    return gain


def normal_values(own_key, shape, scale, limit, pieces=(), kind=jnp.bfloat16):
    array = scale * jax.random.normal(own_key, shape, jnp.float32)
    if pieces:
        array = array * level_of(own_key, shape, pieces, -0.22, 0.18)
    return jnp.clip(array, -limit, limit).astype(kind)


def setup_inputs(seed: int = 0, part: int = 0) -> dict:
    seeds = jax.random.split(jax.random.key(seed), 9)
    part_keys = jax.random.split(jax.random.fold_in(seeds[8], part), 9)
    return {
        "hidden_in": normal_values(part_keys[0], (SEQS, D), 1.0, 6.0),
        "norm_gain": jnp.clip(1.0 + 0.18 * jax.random.normal(part_keys[1], (D,), jnp.float32), 0.1, 1.9),
        "wqkv_old": normal_values(part_keys[2], (N_TP, 2, RANK_COLS, ROWS_OLD), (D // 9) ** -0.5, 0.1875, ((0, 8), (1, 2))),
        "wo": normal_values(part_keys[3], (HEADS * HEAD_DIM, D), (HEADS * HEAD_DIM) ** -0.5, 0.0625, ((0, 16),)),
        "key_cache": draw_key_cache(jax.random.fold_in(jax.random.fold_in(seeds[8], part), 71), part),
        "value_cache": normal_values(part_keys[5], (SEQS, CACHE_LEN, KV_HEADS * HEAD_DIM), 1.0, 6.0, ((1, 16),)),
        "lengths": place_ends(jax.random.randint(part_keys[6], (SEQS,), 1, CACHE_LEN + 1), jax.random.fold_in(part_keys[6], 1), 1, CACHE_LEN).astype(jnp.int32),
        "section_order": jax.random.permutation(part_keys[7], ROW_BLOCKS).astype(jnp.int32),
    }


def rotary(values, positions):
    half = values.shape[-1] // 2
    freqs = 500000.0 ** (-jnp.arange(half, dtype=jnp.float32) * 2.0 / values.shape[-1])
    angles = positions.astype(jnp.float32)[:, None] * freqs[None, :]
    cosine = jnp.cos(angles)[:, None, :]
    sine = jnp.sin(angles)[:, None, :]
    first_half = values[..., :half]
    second_half = values[..., half:]
    return jnp.concatenate([first_half * cosine - second_half * sine, second_half * cosine + first_half * sine], -1)

def rms_normed(hidden_in, norm_gain):
    widened = hidden_in.astype(jnp.float32)
    factor = lax.rsqrt(lax.optimization_barrier(jnp.mean(widened * widened, -1, keepdims=True)) + 1e-05)
    return (widened, (widened * factor * norm_gain).astype(jnp.bfloat16))

def reference(hidden_in, norm_gain, wqkv_old, wo, key_cache, value_cache, lengths, section_order):
    section_count = N_TP // 4
    per_section = ROW_BLOCKS // section_count
    groups = HEADS // KV_HEADS
    q_width = HEADS * HEAD_DIM
    kv_width = KV_HEADS * HEAD_DIM
    by_rank = wqkv_old.reshape(section_count, RANKS, RANK_COLS, per_section, BLOCK_ROWS)
    blocks = jnp.transpose(by_rank, (0, 3, 1, 2, 4)).reshape(ROW_BLOCKS, RANKS, RANK_COLS, BLOCK_ROWS)
    ordered = jnp.zeros_like(blocks).at[section_order].set(blocks)
    full_t = jnp.transpose(ordered, (1, 2, 0, 3)).reshape(QKV, D)
    wqkv_new = jnp.transpose(full_t.reshape(4, 2, section_count, COLS_DEV, D), (2, 0, 1, 3, 4)).reshape(N_TP, 2, COLS_DEV, D)
    widened, normed = rms_normed(hidden_in, norm_gain)
    projected = lax.dot_general(normed, full_t, (((1,), (1,)), ((), ())), preferred_element_type=jnp.float32).astype(jnp.bfloat16)
    queries = rotary(projected[:, :q_width].astype(jnp.float32).reshape(SEQS, HEADS, HEAD_DIM), lengths).astype(jnp.bfloat16)
    new_keys = rotary(projected[:, q_width:q_width + kv_width].astype(jnp.float32).reshape(SEQS, KV_HEADS, HEAD_DIM), lengths).astype(jnp.bfloat16)
    new_values = projected[:, q_width + kv_width:].astype(jnp.float32).reshape(SEQS, KV_HEADS, HEAD_DIM)
    grouped = queries.astype(jnp.float32).reshape(SEQS, KV_HEADS, groups, HEAD_DIM)
    keys_all = key_cache.astype(jnp.float32).reshape(SEQS, CACHE_LEN, KV_HEADS, HEAD_DIM)
    values_all = value_cache.astype(jnp.float32).reshape(SEQS, CACHE_LEN, KV_HEADS, HEAD_DIM)
    inverse = 1.0 / math.sqrt(HEAD_DIM)
    scores = jnp.einsum('bkgd,bpkd->bkgp', grouped, keys_all) * inverse
    usable = (jnp.arange(CACHE_LEN, dtype=jnp.int32)[None, :] < lengths[:, None])[:, None, None, :]
    own_score = lax.optimization_barrier(jnp.sum(grouped * new_keys.astype(jnp.float32)[:, :, None, :], -1)) * inverse
    highest = jnp.maximum(lax.optimization_barrier(jnp.max(jnp.where(usable, scores, -1e+30), -1)), own_score)
    weights = jnp.exp(jnp.where(usable, scores - highest[..., None], -1e+30))
    own_weight = jnp.exp(own_score - highest)
    total = lax.optimization_barrier(jnp.sum(weights, -1)) + own_weight
    mixture = jnp.einsum('bkgp,bpkd->bkgd', weights, values_all) + own_weight[..., None] * new_values[:, :, None, :]
    attended = (mixture / total[..., None]).reshape(SEQS, q_width).astype(jnp.bfloat16)
    mixed_out = (widened + jnp.dot(attended, wo, preferred_element_type=jnp.float32)).astype(jnp.bfloat16)
    return (mixed_out, wqkv_new)
```

```python
import math

import jax
import jax.numpy as jnp
from jax import lax
from jax.experimental import pallas as pl
from jax.experimental.pallas import tpu as pltpu
from jax.sharding import PartitionSpec as P


HEADS = 64
KV_HEADS = 8
HEAD_DIM = 128
RANKS = 8
ROW_BLOCKS = 16
CHUNKS = 16
WAVE_STARTS = (0, 2, 5, 8, 11)


def passed_along(value, axis, steps):
    count = lax.axis_size(axis)
    pairs = [(source, (source + steps) % count) for source in range(count)]
    return lax.ppermute(value, axis, pairs)


def rotary(values, positions):
    half = values.shape[-1] // 2
    freqs = 500000.0 ** (-jnp.arange(half, dtype=jnp.float32) * 2.0 / values.shape[-1])
    angles = positions.astype(jnp.float32)[:, None] * freqs[None, :]
    cosine = jnp.cos(angles)[:, None, :]
    sine = jnp.sin(angles)[:, None, :]
    first_half = values[..., :half]
    second_half = values[..., half:]
    return jnp.concatenate(
        [first_half * cosine - second_half * sine, second_half * cosine + first_half * sine], -1
    )


def rms_normed(hidden_in, norm_gain):
    widened = hidden_in.astype(jnp.float32)
    factor = lax.rsqrt(jnp.mean(widened * widened, -1, keepdims=True) + 1e-05)
    return (widened, (widened * factor * norm_gain).astype(jnp.bfloat16))


def cut_rows(targets, weight, offset, chunk, rows):
    def kernel(target_ref, weight_ref, out_ref):
        out_ref[...] = weight_ref[...]

    shape = (1, 1, rows, weight.shape[3])
    return pl.pallas_call(
        kernel,
        out_shape=jax.ShapeDtypeStruct(shape, weight.dtype),
        grid_spec=pltpu.PrefetchScalarGridSpec(
            num_scalar_prefetch=1,
            grid=(1,),
            in_specs=[
                pl.BlockSpec(shape, lambda step, target_ref: (0, 0, target_ref[offset] + chunk, 0))
            ],
            out_specs=pl.BlockSpec(shape, lambda step, target_ref: (0, 0, 0, 0)),
        ),
        cost_estimate=pl.CostEstimate(
            flops=0, bytes_accessed=4 * rows * weight.shape[3], transcendentals=0
        ),
    )(targets, weight)


def placed_blocks(slots, data, dest, full_shape, offset, per, rows, first_row):
    last = slots.shape[0] - 1
    width = data.shape[-1] // per
    steps = 1 if dest is not None else full_shape[2] // rows

    def kernel(slot_ref, data_ref, *rest):
        out_ref, sems = rest[-2:]
        step = pl.program_id(0)
        at_row = pl.multiple_of(first_row + step * rows, 8)
        copies = []
        for block in range(per):
            column = pl.multiple_of(slot_ref[offset * per + block] * width, width)
            copies.append(
                pltpu.make_async_copy(
                    data_ref.at[0, 0, :, pl.ds(block * width, width)],
                    out_ref.at[0, 0, pl.ds(at_row, rows), pl.ds(column, width)],
                    sems.at[block],
                )
            )
        for copy in copies:
            copy.start()
        for copy in copies:
            copy.wait()

    moved = 2 * steps * rows * data.shape[-1] * 2
    in_specs = [
        pl.BlockSpec(
            (1, 1, rows, data.shape[-1]),
            lambda step, slot_ref: (0, 0, 0 if dest is not None else slot_ref[last] + step, 0),
        )
    ]
    operands = [slots, data]
    aliases = {}
    if dest is not None:
        in_specs.append(pl.BlockSpec(memory_space=pl.ANY))
        operands.append(dest)
        aliases = {2: 0}
    return pl.pallas_call(
        kernel,
        out_shape=jax.ShapeDtypeStruct(full_shape, data.dtype),
        grid_spec=pltpu.PrefetchScalarGridSpec(
            num_scalar_prefetch=1,
            grid=(steps,),
            in_specs=in_specs,
            out_specs=pl.BlockSpec(memory_space=pl.ANY),
            scratch_shapes=[pltpu.SemaphoreType.DMA((per,))],
        ),
        input_output_aliases=aliases,
        cost_estimate=pl.CostEstimate(flops=0, bytes_accessed=moved, transcendentals=0),
    )(*operands)


def shards(hidden_in, norm_gain, wqkv_old, wo, key_cache, value_cache, lengths, section_order):
    tp_count = lax.axis_size("tp")
    sub_count = lax.axis_size("sub")
    device_count = tp_count * sub_count
    section_count = tp_count // 4
    per_section = ROW_BLOCKS // section_count
    tp_index = lax.axis_index("tp")
    sub_index = lax.axis_index("sub")
    own_section = tp_index // 4
    device_rank = tp_index * 2 + sub_index
    cols_dev = wqkv_old.shape[2] // section_count
    rows_old = wqkv_old.shape[3]
    block_rows = rows_old // per_section
    seq_count, width = hidden_in.shape

    chunks = max(1, CHUNKS // max(1, section_count - 1))
    chunk_rows = cols_dev // chunks
    pieces = [(offset, chunk) for chunk in range(chunks) for offset in range(1, section_count)]
    arrived = []

    targets = (own_section + jnp.arange(section_count, dtype=jnp.int32)) % section_count * chunks

    def send_wave(wave):
        first = WAVE_STARTS[wave]
        last = WAVE_STARTS[wave + 1] if wave + 1 < len(WAVE_STARTS) else len(pieces)
        for index in range(first, last):
            offset, chunk = pieces[index]
            outgoing = cut_rows(targets, wqkv_old, offset, chunk, chunk_rows)
            arrived.append((offset, chunk, passed_along(outgoing, "tp", 4 * offset)))

    def exchanged(blocks):
        return lax.all_to_all(blocks, ("tp", "sub"), split_axis=0, concat_axis=0, tiled=True)

    send_wave(0)

    _, normed = rms_normed(hidden_in, norm_gain)
    own_slots = lax.dynamic_slice_in_dim(section_order, own_section * per_section, per_section)
    own_rows = jnp.take(normed.reshape(seq_count, ROW_BLOCKS, block_rows), own_slots, axis=1)
    partial_units = lax.dot_general(
        own_rows.reshape(seq_count, rows_old),
        wqkv_old[0, 0],
        (((1,), (1,)), ((), ())),
        preferred_element_type=jnp.float32,
    )
    send_wave(1)
    gathered = exchanged(
        jnp.broadcast_to(partial_units[None], (device_count,) + partial_units.shape)
    )
    units = jnp.sum(gathered.reshape(section_count, RANKS, seq_count, -1), 0).astype(jnp.bfloat16)
    projected_all = jnp.transpose(units, (1, 0, 2)).reshape(seq_count, -1)

    q_width = HEADS * HEAD_DIM
    kv_width = KV_HEADS * HEAD_DIM
    groups = HEADS // KV_HEADS
    queries = rotary(
        projected_all[:, :q_width].astype(jnp.float32).reshape(seq_count, HEADS, HEAD_DIM), lengths
    ).astype(jnp.bfloat16)
    new_keys = rotary(
        projected_all[:, q_width : q_width + kv_width]
        .astype(jnp.float32)
        .reshape(seq_count, KV_HEADS, HEAD_DIM),
        lengths,
    ).astype(jnp.bfloat16)
    new_values = (
        projected_all[:, q_width + kv_width :]
        .astype(jnp.float32)
        .reshape(seq_count, KV_HEADS, HEAD_DIM)
    )
    pos_count = key_cache.shape[1]
    positions = device_rank * pos_count + jnp.arange(pos_count, dtype=jnp.int32)
    usable = (positions[None, :] < lengths[:, None])[:, None, None, :]
    inverse = 1.0 / math.sqrt(HEAD_DIM)
    grouped = queries.reshape(seq_count, KV_HEADS, groups, HEAD_DIM)
    keys_local = key_cache.reshape(seq_count, pos_count, KV_HEADS, HEAD_DIM)
    values_local = value_cache.reshape(seq_count, pos_count, KV_HEADS, HEAD_DIM).astype(jnp.float32)
    scores = (
        jnp.einsum("bkgd,bpkd->bkgp", grouped, keys_local, preferred_element_type=jnp.float32)
        * inverse
    )
    local_top = jnp.max(jnp.where(usable, scores, -1e30), -1)
    weights = jnp.exp(jnp.where(usable, scores - local_top[..., None], -1e30))
    local_sum = jnp.sum(weights, -1).reshape(seq_count, HEADS)
    local_mix = jnp.einsum("bkgp,bpkd->bkgd", weights, values_local).reshape(
        seq_count, HEADS, HEAD_DIM
    )
    local_top = local_top.reshape(seq_count, HEADS)
    heads_dev = wo.shape[0] // HEAD_DIM
    first_head = device_rank * heads_dev
    half = HEAD_DIM // 2
    spread = (seq_count, HEADS, half)
    packed = jnp.concatenate(
        [
            local_mix,
            jnp.broadcast_to(local_top[..., None], spread),
            jnp.broadcast_to(local_sum[..., None], spread),
        ],
        -1,
    )
    packed = jnp.transpose(
        packed.reshape(seq_count, device_count, heads_dev, 2 * HEAD_DIM), (1, 0, 2, 3)
    ).reshape(device_count, seq_count * heads_dev, 2 * HEAD_DIM)
    send_wave(2)
    parts_in = exchanged(packed)
    parts_in = parts_in.reshape(device_count, seq_count, heads_dev, 2 * HEAD_DIM)
    mixes_in = parts_in[..., :HEAD_DIM]
    tops_in = parts_in[..., HEAD_DIM]
    sums_in = parts_in[..., HEAD_DIM + half]
    best = jnp.max(tops_in, 0)
    factors = jnp.exp(tops_in - best[None])
    head_sum = jnp.sum(sums_in * factors, 0)
    head_mix = jnp.sum(mixes_in * factors[..., None], 0)
    own_queries = lax.dynamic_slice_in_dim(queries, first_head, heads_dev, 1).astype(jnp.float32)
    kv_index = (first_head + jnp.arange(heads_dev, dtype=jnp.int32)) // groups
    own_keys = jnp.take(new_keys, kv_index, axis=1).astype(jnp.float32)
    own_values = jnp.take(new_values, kv_index, axis=1)
    own_score = jnp.sum(own_queries * own_keys, -1) * inverse
    highest = jnp.maximum(best, own_score)
    old_scale = jnp.exp(best - highest)
    own_weight = jnp.exp(own_score - highest)
    numerator = head_mix * old_scale[..., None] + own_weight[..., None] * own_values
    denominator = head_sum * old_scale + own_weight
    attended = (
        (numerator / denominator[..., None])
        .reshape(seq_count, heads_dev * HEAD_DIM)
        .astype(jnp.bfloat16)
    )
    partial_out = jnp.dot(attended, wo, preferred_element_type=jnp.float32)
    share = width // device_count
    by_owner = jnp.transpose(partial_out.reshape(seq_count, device_count, share), (1, 0, 2))
    send_wave(3)
    shares_in = exchanged(by_owner)
    own_hidden = lax.dynamic_slice_in_dim(hidden_in, device_rank * share, share, 1)
    own_out = (own_hidden.astype(jnp.float32) + jnp.sum(shares_in, 0)).astype(jnp.bfloat16)
    send_wave(4)
    all_out = exchanged(jnp.broadcast_to(own_out[None], (device_count,) + own_out.shape))
    mixed_out = jnp.transpose(all_out, (1, 0, 2)).reshape(seq_count, width)

    full_shape = (1, 1, cols_dev, ROW_BLOCKS * block_rows)
    sources = (own_section - jnp.arange(section_count, dtype=jnp.int32)) % section_count
    slots = jnp.concatenate(
        [
            jnp.take(section_order.reshape(section_count, per_section), sources, axis=0).reshape(-1),
            (own_section * chunks)[None].astype(jnp.int32),
        ]
    )
    new_weight = placed_blocks(
        slots, wqkv_old, None, full_shape, 0, per_section, chunk_rows, 0
    )
    for offset, chunk, data in arrived:
        new_weight = placed_blocks(
            slots,
            data,
            new_weight,
            full_shape,
            offset,
            per_section,
            chunk_rows,
            chunk * chunk_rows,
        )
    return (mixed_out, new_weight)


def solution(mesh):
    placed = (
        P("replica", None),
        P("replica"),
        P(("replica", "tp"), "sub", None, None),
        P(("replica", "tp", "sub"), None),
        P("replica", ("tp", "sub"), None),
        P("replica", ("tp", "sub"), None),
        P("replica"),
        P("replica"),
    )

    return jax.shard_map(
        shards,
        mesh=mesh,
        in_specs=placed,
        out_specs=(P("replica", None), P(("replica", "tp"), "sub", None, None)),
        check_vma=False,
    )
```

```python
import math

import jax
import jax.numpy as jnp
from jax import lax
from jax.experimental import pallas as pl
from jax.experimental.pallas import tpu as pltpu
from jax.sharding import PartitionSpec as P


HEADS = 64
KV_HEADS = 8
HEAD_DIM = 128
RANKS = 8
ROW_BLOCKS = 16
CHUNKS = 16
WAVE_STARTS = (0, 2, 6, 10, 13)


def passed_along(value, axis, steps):
    count = lax.axis_size(axis)
    pairs = [(source, (source + steps) % count) for source in range(count)]
    return lax.ppermute(value, axis, pairs)


def rotary(values, positions):
    half = values.shape[-1] // 2
    freqs = 500000.0 ** (-jnp.arange(half, dtype=jnp.float32) * 2.0 / values.shape[-1])
    angles = positions.astype(jnp.float32)[:, None] * freqs[None, :]
    cosine = jnp.cos(angles)[:, None, :]
    sine = jnp.sin(angles)[:, None, :]
    first_half = values[..., :half]
    second_half = values[..., half:]
    return jnp.concatenate(
        [first_half * cosine - second_half * sine, second_half * cosine + first_half * sine], -1
    )


def rms_normed(hidden_in, norm_gain):
    widened = hidden_in.astype(jnp.float32)
    factor = lax.rsqrt(jnp.mean(widened * widened, -1, keepdims=True) + 1e-05)
    return (widened, (widened * factor * norm_gain).astype(jnp.bfloat16))


def cut_rows(targets, weight, offset, chunk, rows):
    def kernel(target_ref, weight_ref, out_ref):
        out_ref[...] = weight_ref[...]

    shape = (1, 1, rows, weight.shape[3])
    return pl.pallas_call(
        kernel,
        out_shape=jax.ShapeDtypeStruct(shape, weight.dtype),
        grid_spec=pltpu.PrefetchScalarGridSpec(
            num_scalar_prefetch=1,
            grid=(1,),
            in_specs=[
                pl.BlockSpec(shape, lambda step, target_ref: (0, 0, target_ref[offset] + chunk, 0))
            ],
            out_specs=pl.BlockSpec(shape, lambda step, target_ref: (0, 0, 0, 0)),
        ),
        cost_estimate=pl.CostEstimate(
            flops=0, bytes_accessed=4 * rows * weight.shape[3], transcendentals=0
        ),
    )(targets, weight)


def joined(shares):
    count, seq_count, share = shares.shape

    def kernel(share_ref, out_ref):
        for index in range(count):
            out_ref[:, index * share : (index + 1) * share] = share_ref[index]

    return pl.pallas_call(
        kernel,
        out_shape=jax.ShapeDtypeStruct((seq_count, count * share), shares.dtype),
    )(shares)


def placed_blocks(slots, data, dest, full_shape, offset, per, rows, first_row):
    last = slots.shape[0] - 1
    width = data.shape[-1] // per
    steps = 1 if dest is not None else full_shape[2] // rows

    def kernel(slot_ref, data_ref, *rest):
        out_ref, sems = rest[-2:]
        step = pl.program_id(0)
        at_row = pl.multiple_of(first_row + step * rows, 8)
        copies = []
        for block in range(per):
            column = pl.multiple_of(slot_ref[offset * per + block] * width, width)
            copies.append(
                pltpu.make_async_copy(
                    data_ref.at[0, 0, :, pl.ds(block * width, width)],
                    out_ref.at[0, 0, pl.ds(at_row, rows), pl.ds(column, width)],
                    sems.at[block],
                )
            )
        for copy in copies:
            copy.start()
        for copy in copies:
            copy.wait()

    moved = 2 * steps * rows * data.shape[-1] * 2
    in_specs = [
        pl.BlockSpec(
            (1, 1, rows, data.shape[-1]),
            lambda step, slot_ref: (0, 0, 0 if dest is not None else slot_ref[last] + step, 0),
        )
    ]
    operands = [slots, data]
    aliases = {}
    if dest is not None:
        in_specs.append(pl.BlockSpec(memory_space=pl.ANY))
        operands.append(dest)
        aliases = {2: 0}
    return pl.pallas_call(
        kernel,
        out_shape=jax.ShapeDtypeStruct(full_shape, data.dtype),
        grid_spec=pltpu.PrefetchScalarGridSpec(
            num_scalar_prefetch=1,
            grid=(steps,),
            in_specs=in_specs,
            out_specs=pl.BlockSpec(memory_space=pl.ANY),
            scratch_shapes=[pltpu.SemaphoreType.DMA((per,))],
        ),
        input_output_aliases=aliases,
        cost_estimate=pl.CostEstimate(flops=0, bytes_accessed=moved, transcendentals=0),
    )(*operands)


def shards(hidden_in, norm_gain, wqkv_old, wo, key_cache, value_cache, lengths, section_order):
    tp_count = lax.axis_size("tp")
    sub_count = lax.axis_size("sub")
    device_count = tp_count * sub_count
    section_count = tp_count // 4
    per_section = ROW_BLOCKS // section_count
    tp_index = lax.axis_index("tp")
    sub_index = lax.axis_index("sub")
    own_section = tp_index // 4
    device_rank = tp_index * 2 + sub_index
    cols_dev = wqkv_old.shape[2] // section_count
    rows_old = wqkv_old.shape[3]
    block_rows = rows_old // per_section
    seq_count, width = hidden_in.shape

    chunks = max(1, CHUNKS // max(1, section_count - 1))
    chunk_rows = cols_dev // chunks
    pieces = [(offset, chunk) for chunk in range(chunks) for offset in range(1, section_count)]
    arrived = []

    targets = (own_section + jnp.arange(section_count, dtype=jnp.int32)) % section_count * chunks

    def send_wave(wave):
        first = WAVE_STARTS[wave]
        last = WAVE_STARTS[wave + 1] if wave + 1 < len(WAVE_STARTS) else len(pieces)
        for index in range(first, last):
            offset, chunk = pieces[index]
            outgoing = cut_rows(targets, wqkv_old, offset, chunk, chunk_rows)
            arrived.append((offset, chunk, passed_along(outgoing, "tp", 4 * offset)))

    def exchanged(blocks):
        return lax.all_to_all(blocks, ("tp", "sub"), split_axis=0, concat_axis=0, tiled=True)

    send_wave(0)

    _, normed = rms_normed(hidden_in, norm_gain)
    own_slots = lax.dynamic_slice_in_dim(section_order, own_section * per_section, per_section)
    own_rows = jnp.take(normed.reshape(seq_count, ROW_BLOCKS, block_rows), own_slots, axis=1)
    partial_units = lax.dot_general(
        own_rows.reshape(seq_count, rows_old),
        wqkv_old[0, 0],
        (((1,), (1,)), ((), ())),
        preferred_element_type=jnp.float32,
    )
    send_wave(1)
    gathered = exchanged(
        jnp.broadcast_to(partial_units[None], (device_count,) + partial_units.shape)
    )
    units = jnp.sum(gathered.reshape(section_count, RANKS, seq_count, -1), 0).astype(jnp.bfloat16)
    projected_all = jnp.transpose(units, (1, 0, 2)).reshape(seq_count, -1)

    q_width = HEADS * HEAD_DIM
    kv_width = KV_HEADS * HEAD_DIM
    groups = HEADS // KV_HEADS
    queries = rotary(
        projected_all[:, :q_width].astype(jnp.float32).reshape(seq_count, HEADS, HEAD_DIM), lengths
    ).astype(jnp.bfloat16)
    new_keys = rotary(
        projected_all[:, q_width : q_width + kv_width]
        .astype(jnp.float32)
        .reshape(seq_count, KV_HEADS, HEAD_DIM),
        lengths,
    ).astype(jnp.bfloat16)
    new_values = (
        projected_all[:, q_width + kv_width :]
        .astype(jnp.float32)
        .reshape(seq_count, KV_HEADS, HEAD_DIM)
    )
    pos_count = key_cache.shape[1]
    positions = device_rank * pos_count + jnp.arange(pos_count, dtype=jnp.int32)
    usable = (positions[None, :] < lengths[:, None])[:, None, None, :]
    inverse = 1.0 / math.sqrt(HEAD_DIM)
    grouped = queries.reshape(seq_count, KV_HEADS, groups, HEAD_DIM)
    keys_local = key_cache.reshape(seq_count, pos_count, KV_HEADS, HEAD_DIM)
    values_local = value_cache.reshape(seq_count, pos_count, KV_HEADS, HEAD_DIM).astype(jnp.float32)
    scores = (
        jnp.einsum("bkgd,bpkd->bkgp", grouped, keys_local, preferred_element_type=jnp.float32)
        * inverse
    )
    local_top = jnp.max(jnp.where(usable, scores, -1e30), -1)
    weights = jnp.exp(jnp.where(usable, scores - local_top[..., None], -1e30))
    local_sum = jnp.sum(weights, -1).reshape(seq_count, HEADS)
    local_mix = jnp.einsum("bkgp,bpkd->bkgd", weights, values_local).reshape(
        seq_count, HEADS, HEAD_DIM
    )
    local_top = local_top.reshape(seq_count, HEADS)
    heads_dev = wo.shape[0] // HEAD_DIM
    first_head = device_rank * heads_dev
    half = HEAD_DIM // 2
    spread = (seq_count, HEADS, half)
    packed = jnp.concatenate(
        [
            local_mix,
            jnp.broadcast_to(local_top[..., None], spread),
            jnp.broadcast_to(local_sum[..., None], spread),
        ],
        -1,
    )
    packed = jnp.transpose(
        packed.reshape(seq_count, device_count, heads_dev, 2 * HEAD_DIM), (1, 0, 2, 3)
    ).reshape(device_count, seq_count * heads_dev, 2 * HEAD_DIM)
    send_wave(2)
    parts_in = exchanged(packed)
    parts_in = parts_in.reshape(device_count, seq_count, heads_dev, 2 * HEAD_DIM)
    mixes_in = parts_in[..., :HEAD_DIM]
    tops_in = parts_in[..., HEAD_DIM]
    sums_in = parts_in[..., HEAD_DIM + half]
    best = jnp.max(tops_in, 0)
    factors = jnp.exp(tops_in - best[None])
    head_sum = jnp.sum(sums_in * factors, 0)
    head_mix = jnp.sum(mixes_in * factors[..., None], 0)
    own_queries = lax.dynamic_slice_in_dim(queries, first_head, heads_dev, 1).astype(jnp.float32)
    kv_index = (first_head + jnp.arange(heads_dev, dtype=jnp.int32)) // groups
    own_keys = jnp.take(new_keys, kv_index, axis=1).astype(jnp.float32)
    own_values = jnp.take(new_values, kv_index, axis=1)
    own_score = jnp.sum(own_queries * own_keys, -1) * inverse
    highest = jnp.maximum(best, own_score)
    old_scale = jnp.exp(best - highest)
    own_weight = jnp.exp(own_score - highest)
    numerator = head_mix * old_scale[..., None] + own_weight[..., None] * own_values
    denominator = head_sum * old_scale + own_weight
    attended = (
        (numerator / denominator[..., None])
        .reshape(seq_count, heads_dev * HEAD_DIM)
        .astype(jnp.bfloat16)
    )
    partial_out = jnp.dot(attended, wo, preferred_element_type=jnp.float32)
    share = width // device_count
    by_owner = jnp.transpose(partial_out.reshape(seq_count, device_count, share), (1, 0, 2))
    send_wave(3)
    shares_in = exchanged(by_owner)
    own_hidden = lax.dynamic_slice_in_dim(hidden_in, device_rank * share, share, 1)
    own_out = (own_hidden.astype(jnp.float32) + jnp.sum(shares_in, 0)).astype(jnp.bfloat16)
    send_wave(4)
    all_out = exchanged(jnp.broadcast_to(own_out[None], (device_count,) + own_out.shape))
    mixed_out = joined(all_out)

    full_shape = (1, 1, cols_dev, ROW_BLOCKS * block_rows)
    sources = (own_section - jnp.arange(section_count, dtype=jnp.int32)) % section_count
    slots = jnp.concatenate(
        [
            jnp.take(section_order.reshape(section_count, per_section), sources, axis=0).reshape(-1),
            (own_section * chunks)[None].astype(jnp.int32),
        ]
    )
    new_weight = placed_blocks(
        slots, wqkv_old, None, full_shape, 0, per_section, chunk_rows, 0
    )
    for offset, chunk, data in arrived:
        new_weight = placed_blocks(
            slots,
            data,
            new_weight,
            full_shape,
            offset,
            per_section,
            chunk_rows,
            chunk * chunk_rows,
        )
    return (mixed_out, new_weight)


def solution(mesh):
    placed = (
        P("replica", None),
        P("replica"),
        P(("replica", "tp"), "sub", None, None),
        P(("replica", "tp", "sub"), None),
        P("replica", ("tp", "sub"), None),
        P("replica", ("tp", "sub"), None),
        P("replica"),
        P("replica"),
    )

    return jax.shard_map(
        shards,
        mesh=mesh,
        in_specs=placed,
        out_specs=(P("replica", None), P(("replica", "tp"), "sub", None, None)),
        check_vma=False,
    )
```
